32 devices in a mesh: seq: 4 (over y, x), exp: 8 (over z, core), dp: 1.
Axes of the slice: x: 2, y: 2, z: 4, core: 2. Of those that a mesh axis runs over, the one named last changes fastest.
Arguments:
- tokens: bfloat16 [8, 16, 64, 1280], P(('dp', 'exp'), 'seq'), may hold values from -6 to 6
- expert_ids: int32 [8, 16, 64, 1], P(('dp', 'exp'), 'seq'), may hold values from 0 to 15; in each aligned block of 256 rows (0 to 255, 256 to 511, ..., all dimensions but the last counted through in order) at most 20 rows name the same one
- gate_values: float32 [8, 16, 64], P(('dp', 'exp'), 'seq'), may hold values from 0.25 to 1
- mixer_gain: float32 [1280], replicated, may hold values from 0.1 to 1.9
- expert_gain: float32 [1280], replicated, may hold values from 0.1 to 1.9
- conv_weight: float32 [3, 3, 1280], replicated, may hold values from -2 to 2
- conv_bias: float32 [1280], replicated, may hold values from -3 to 3
- w_in: bfloat16 [16, 1280, 5120], P('exp', None, 'seq'), may hold values from -0.15625 to 0.15625
- b_in: float32 [16, 5120], P('exp', 'seq'), may hold values from -3 to 3
- w_out: bfloat16 [16, 5120, 1280], P('exp', 'seq'), may hold values from -0.078125 to 0.078125
- b_out: float32 [16, 1280], P('exp'), may hold values from -3 to 3
Outputs:
- result: bfloat16 [8, 16, 64, 1280], P(('dp', 'exp'), 'seq')
The draws below stay inside these ranges and needn't reach their ends.
Inputs may be any that keep to these rules, and one draw needn't show every extreme that they name: `expert_ids`: among the 256 patches of one image's block of 4 rows (rows k * 4 to k * 4 + 3), no expert is chosen more than 20 times, and in every draw some expert is chosen exactly 20 times in some block.
All inputs are finite; a program needn't handle non-finite values.
Results may differ from the reference program's by a relative error of at most 0.006.
Values may be sent and summed in bfloat16 or wider, within the bound.
A program may use at most 128 MiB of HBM per device.

```python
import math
import jax
import jax.numpy as jnp
import numpy as np
from jax import lax

D = 1280
FF = 5120
WIDTH = 64
EXPERTS = 16
HEIGHT = 16
IMAGES = 8
TOK_DEV = 256
CAP = 20
N_SEQ = 4


def steps_of(stream_key, extent, split, low, largest):
    level = 1.0
    for dim, shards_of in split:
        heights = jax.random.uniform(jax.random.fold_in(jax.random.fold_in(stream_key, 6), dim), (shards_of,), jnp.float32, low / len(split), largest / len(split))
        level = level * jnp.repeat(jnp.exp(heights), extent[dim] // shards_of).reshape((-1,) + (1,) * (len(extent) - 1 - dim))
    return level


def shared_out(key, own, number, rows, amount, top, limit, slope):
    sequence = jax.random.permutation(key, amount)
    packed, usual = load_shares(amount, rows * top, limit, slope, True), load_shares(amount, rows * top, limit, slope, False)
    places = jnp.arange(amount)

    def named(tallies, rotation):
        used = int((tallies > 0).sum())
        fixed = max(1, used // 4)
        passed = fixed + (places - fixed + rotation * (used - fixed)) % max(1, amount - fixed)
        return jnp.zeros((amount,), jnp.int32).at[sequence[jnp.where(places < fixed, places, passed)]].set(jnp.asarray(tallies, jnp.int32))

    tallies = jnp.where(number % 4 == 0, named(packed, number // 4), named(usual, number - number // 4 - 1))
    mixed = jax.random.permutation(jax.random.fold_in(own, 3), amount)
    source_of, taker = mixed[0:amount // 2 * 2:2], mixed[1:amount // 2 * 2:2]
    margin = jnp.minimum(tallies[source_of] - 1, limit - tallies[taker]) // 2
    margin = jnp.where((source_of == sequence[0]) | (taker == sequence[0]) | (tallies[taker] == 0), 0, jnp.maximum(margin, 0))
    passed = jax.random.randint(jax.random.fold_in(own, 4), (amount // 2,), 0, 1 << 20) % (margin + 1)
    tallies = tallies.at[source_of].add(-passed).at[taker].add(passed)
    labels = jnp.searchsorted(jnp.cumsum(tallies), jnp.arange(rows * top), side="right").astype(jnp.int32)
    grid = labels.reshape(top, rows).T
    grid = grid[jax.random.permutation(jax.random.fold_in(own, 1), rows)]
    rotation = jax.random.randint(jax.random.fold_in(own, 2), (rows, 1), 0, top)
    return jnp.take_along_axis(grid, (jnp.arange(top)[None, :] + rotation) % top, axis=1)


def load_shares(number_of, total, limit, skew, full):
    portions = [(1 << 20) // math.isqrt(rank ** skew) + 1 for rank in range(1, number_of + 1)]
    largest = limit if full else min(limit, max(-(-total // number_of), total * portions[0] // sum(portions)))
    least = 1 if total - largest >= number_of - 1 else 0
    given, spare = [largest] + [least] * (number_of - 1), total - largest - least * (number_of - 1)
    while spare > 0:
        candidates = [i for i in range(1, number_of) if given[i] < largest] or [i for i in range(1, number_of) if given[i] < limit]
        mass, budget = sum([portions[i] for i in candidates]), spare
        for i in candidates:
            addition = min(limit - given[i], max(1, budget * portions[i] // mass), spare)
            given[i] = given[i] + addition
            spare = spare - addition
    return np.array(given)


def normal_values(own_key, dims, deviation, most, pieces=(), kind=jnp.bfloat16):
    values = deviation * jax.random.normal(own_key, dims, jnp.float32)
    if pieces:
        values = values * steps_of(own_key, dims, pieces, -0.22, 0.18)
    return jnp.clip(values, -most, most).astype(kind)


def setup_inputs(seed: int = 0, part: int = 0) -> dict:
    keys = jax.random.split(jax.random.key(seed), 12)
    part_keys = jax.random.split(jax.random.fold_in(keys[11], part), 12)
    tokens = normal_values(part_keys[0], (IMAGES, HEIGHT, WIDTH, D), 1.0, 6.0, ((0, 8), (1, 4)))
    expert_ids_keys = jax.random.split(jax.random.fold_in(part_keys[1], 1), IMAGES * HEIGHT * WIDTH // TOK_DEV)
    expert_ids_turns = jax.random.permutation(jax.random.fold_in(part_keys[1], 3), IMAGES * HEIGHT * WIDTH // TOK_DEV)
    expert_ids = jax.vmap(lambda own, number: shared_out(jax.random.fold_in(part_keys[1], 2), own, number, TOK_DEV, EXPERTS, 1, CAP, 2))(expert_ids_keys, expert_ids_turns).reshape((IMAGES, HEIGHT, WIDTH, 1))
    gate_values = jnp.clip(jnp.exp(math.log(1.0) - 1.3862944 * jax.random.uniform(part_keys[2], (IMAGES, HEIGHT, WIDTH), jnp.float32) ** steps_of(part_keys[2], (IMAGES, HEIGHT, WIDTH), ((0, 8), (1, 4)), -0.2, 0.2)), 0.25, 1.0)
    mixer_gain = jnp.clip(1.0 + 0.18 * jax.random.normal(keys[3], (D,), jnp.float32), 0.1, 1.9)
    expert_gain = jnp.clip(1.0 + 0.18 * jax.random.normal(keys[4], (D,), jnp.float32), 0.1, 1.9)
    conv_weight = normal_values(keys[5], (3, 3, D), 9 ** -0.5, 2.0, (), jnp.float32)
    conv_bias = normal_values(keys[6], (D,), 0.5, 3.0, (), jnp.float32)
    w_in = normal_values(keys[7], (EXPERTS, D, FF), D ** -0.5, 0.15625, ((0, 8), (2, 4)))
    b_in = normal_values(keys[8], (EXPERTS, FF), 0.5, 3.0, ((0, 8), (1, 4)), jnp.float32)
    w_out = normal_values(keys[9], (EXPERTS, FF, D), FF ** -0.5, 0.078125, ((0, 8), (1, 4)))
    b_out = normal_values(keys[10], (EXPERTS, D), 0.5, 3.0, ((0, 8),), jnp.float32)
    return dict(tokens=tokens, expert_ids=expert_ids, gate_values=gate_values, mixer_gain=mixer_gain, expert_gain=expert_gain, conv_weight=conv_weight, conv_bias=conv_bias, w_in=w_in, b_in=b_in, w_out=w_out, b_out=b_out)


def normalize(values, scales):
    row_mean = lax.optimization_barrier(jnp.mean(values, axis=-1, keepdims=True))
    centred = values - row_mean
    row_var = lax.optimization_barrier(jnp.mean(centred * centred, axis=-1, keepdims=True))
    return centred * lax.rsqrt(row_var + 1e-06) * scales

def depthwise(padded, conv_weight, height, width):
    summed = padded[..., 0:height, 0:width, :] * conv_weight[0, 0]
    for row_off in range(3):
        for col_off in range(3):
            if row_off + col_off > 0:
                summed = summed + padded[..., row_off:row_off + height, col_off:col_off + width, :] * conv_weight[row_off, col_off]
    return summed

def reference(tokens, expert_ids, gate_values, mixer_gain, expert_gain, conv_weight, conv_bias, w_in, b_in, w_out, b_out):
    values = tokens.astype(jnp.float32)
    mixer_in = normalize(values, mixer_gain).astype(jnp.bfloat16).astype(jnp.float32)
    padded = jnp.pad(mixer_in, ((0, 0), (1, 1), (1, 1), (0, 0)))
    mixed = values + depthwise(padded, conv_weight, HEIGHT, WIDTH) + conv_bias
    expert_in = normalize(mixed, expert_gain).astype(jnp.bfloat16).reshape(-1, D)
    blocks = IMAGES * N_SEQ
    route_ids = expert_ids.reshape(blocks, TOK_DEV).astype(jnp.int32)
    one_hot = (route_ids[:, :, None] == jnp.arange(EXPERTS, dtype=jnp.int32)[None, None, :]).astype(jnp.int32)
    slot_rank = lax.optimization_barrier(jnp.sum(one_hot * (jnp.cumsum(one_hot, axis=1) - 1), axis=2)).astype(jnp.int32)
    slot_index = (jnp.arange(blocks, dtype=jnp.int32)[:, None] * CAP + slot_rank).reshape(-1).astype(jnp.int32)
    flat_ids = route_ids.reshape(-1)
    buffer = jnp.zeros((EXPERTS, blocks * CAP, D), jnp.bfloat16).at[flat_ids, slot_index].set(expert_in)
    piece_width = FF // N_SEQ

    def expert_pass(inputs):
        rows, first, first_bias, second, second_bias = inputs
        summed = jnp.zeros((rows.shape[0], D), jnp.float32)
        for shard in range(N_SEQ):
            low = shard * piece_width
            hidden = jnp.dot(rows, first[:, low:low + piece_width], preferred_element_type=jnp.float32) + first_bias[low:low + piece_width]
            hidden = jax.nn.gelu(hidden, approximate=False).astype(jnp.bfloat16)
            partial_sum = jnp.dot(hidden, second[low:low + piece_width], preferred_element_type=jnp.float32)
            summed = summed + partial_sum.astype(jnp.bfloat16).astype(jnp.float32)
        return (summed + second_bias).astype(jnp.bfloat16)
    expert_out = lax.map(expert_pass, (buffer, w_in, b_in, w_out, b_out))
    picked = expert_out[flat_ids, slot_index].astype(jnp.float32)
    result = mixed.reshape(-1, D) + gate_values.reshape(-1)[:, None] * picked
    return result.astype(jnp.bfloat16).reshape(IMAGES, HEIGHT, WIDTH, D)
```

```python
import functools
import math

import jax
import jax.numpy as jnp
from jax import lax
from jax.experimental import pallas as pl
from jax.experimental.pallas import tpu as pltpu
from jax.sharding import PartitionSpec as P


def with_halo(cells, sides, width):
    for axis, dim in sides:
        count = lax.axis_size(axis)
        ends = count - 1
        head = lax.slice_in_dim(cells, 0, width, axis=dim)
        tail = lax.slice_in_dim(cells, cells.shape[dim] - width, cells.shape[dim], axis=dim)
        cells = jnp.concatenate(
            [
                lax.ppermute(tail, axis, [(i, (i + 1) % count) for i in range(ends)]),
                cells,
                lax.ppermute(head, axis, [((i + 1) % count, i) for i in range(ends)]),
            ],
            axis=dim,
        )
    return cells


def normalize(values, scales):
    row_mean = jnp.mean(values, axis=-1, keepdims=True)
    centred = values - row_mean
    row_var = jnp.mean(centred * centred, axis=-1, keepdims=True)
    return centred * lax.rsqrt(row_var + 1e-06) * scales


def depthwise(padded, conv_weight, height, width):
    summed = padded[..., 0:height, 0:width, :] * conv_weight[0, 0]
    for row_off in range(3):
        for col_off in range(3):
            if row_off + col_off > 0:
                summed = (
                    summed
                    + padded[..., row_off : row_off + height, col_off : col_off + width, :]
                    * conv_weight[row_off, col_off]
                )
    return summed


VMEM_LIMIT = 62 * 1024 * 1024
MESH = pl.DeviceIdType.MESH


def exchange_kernel(
    dims,
    x_ref,
    b_in_ref,
    b_out_ref,
    w_in_ref,
    w_out_ref,
    out_ref,
    w1,
    w2,
    buf,
    part,
    got1,
    red,
    got2,
    fin,
    xs,
    hs,
    w_sem,
    own_sem,
    z_send,
    z_recv,
    a1_send,
    a1_recv,
    a2_send,
    a2_recv,
    r1_send,
    r1_recv,
    r2_send,
    r2_recv,
    b_send,
    b_recv,
):
    n_seq, n_exp, n_chunk, pair, major, minor, experts, slot = dims
    groups = x_ref.shape[1]
    width = x_ref.shape[3]
    hidden = w1.shape[2]
    me_s = lax.axis_index("seq")
    me_e = lax.axis_index("exp")
    me_z = me_e // pair
    me_c = me_e % pair

    def place(h):
        if major == minor and h % 2 == 1:
            return me_s % minor, me_s // minor
        return me_s // minor, me_s % minor

    def at(h, maj, low):
        if major == minor and h % 2 == 1:
            return low * minor + maj
        return maj * minor + low

    def remote(src, dst, send, recv, seq, exp):
        return pltpu.make_async_remote_copy(
            src_ref=src,
            dst_ref=dst,
            send_sem=send,
            recv_sem=recv,
            device_id={"seq": seq, "exp": exp},
            device_id_type=MESH,
        )

    weights = []
    for j in range(experts):
        weights.append(pltpu.make_async_copy(w_in_ref.at[j], w1.at[j], w_sem.at[0, j]))
    for j in range(experts):
        weights.append(pltpu.make_async_copy(w_out_ref.at[j], w2.at[j], w_sem.at[1, j]))

    barrier = pltpu.get_barrier_semaphore()
    greeted = 0
    for d in range(1, n_exp):
        pl.semaphore_signal(
            barrier,
            inc=1,
            device_id={"seq": me_s, "exp": (me_e + d) % n_exp},
            device_id_type=MESH,
        )
        greeted += 1
    for h in range(min(pair, 2) if major == minor else 1):
        maj, low = place(h)
        for d in range(1, minor):
            pl.semaphore_signal(
                barrier,
                inc=1,
                device_id={"seq": at(h, maj, (low + d) % minor), "exp": me_e},
                device_id_type=MESH,
            )
            greeted += 1
        if pair == 1:
            for d in range(1, major):
                pl.semaphore_signal(
                    barrier,
                    inc=1,
                    device_id={"seq": at(h, (maj + d) % major, low), "exp": me_e},
                    device_id_type=MESH,
                )
                greeted += 1
    pl.semaphore_wait(barrier, greeted)

    def z_copy(c, h):
        target = (me_z + c) % n_chunk * pair + (me_c + pair - h) % pair
        maj, low = place(h)
        return remote(
            x_ref.at[target],
            buf.at[c, h, maj, low],
            z_send.at[c, h],
            z_recv.at[c, h],
            me_s,
            target,
        )

    own_maj, own_low = place(0)
    own = pltpu.make_async_copy(x_ref.at[me_e], buf.at[0, 0, own_maj, own_low], own_sem)

    def a1_copy(c, h, d):
        maj, low = place(h)
        block = buf.at[c, h, maj, low]
        return remote(
            block,
            block,
            a1_send.at[c, h, d],
            a1_recv.at[c, h, d],
            at(h, maj, (low + d) % minor),
            me_e,
        )

    def a2_copy(c, h, d):
        maj, low = place(h)
        block = buf.at[c, h, maj]
        return remote(
            block,
            block,
            a2_send.at[c, h, d],
            a2_recv.at[c, h, d],
            at(h, (maj + d) % major, low),
            me_e,
        )

    def r1_copy(c, h, d):
        maj, low = place(h)
        return remote(
            part.at[c, h, (maj + d) % major],
            got1.at[c, h, d - 1],
            r1_send.at[c, h, d],
            r1_recv.at[c, h, d],
            at(h, (maj + d) % major, low),
            me_e,
        )

    def r2_copy(c, h, d):
        maj, low = place(h)
        return remote(
            red.at[c, h, (low + d) % minor],
            got2.at[c, h, d - 1],
            r2_send.at[c, h, d],
            r2_recv.at[c, h, d],
            at(h, maj, (low + d) % minor),
            me_e,
        )

    def b_copy(c, h):
        target = (me_z + n_chunk - c) % n_chunk * pair + (me_c + h) % pair
        return remote(
            fin.at[c, h],
            out_ref.at[me_e],
            b_send.at[c, h],
            b_recv.at[c, h],
            me_s,
            target,
        )

    def gather_near(c):
        for h in range(pair):
            if c == 0 and h == 0:
                own.wait()
            else:
                z_copy(c, h).wait_recv()
            for d in range(1, minor):
                a1_copy(c, h, d).start()

    def gather_far(c):
        for h in range(pair):
            for d in range(1, minor):
                a1_copy(c, h, d).wait_recv()
            for d in range(1, major):
                a2_copy(c, h, d).start()

    spans = []
    for j in range(experts):
        spans.append((j * slot // 8, -(-(j + 1) * slot // 8)))

    blocks = [(h, i, k) for h in range(pair) for i in range(major) for k in range(minor)]

    def compute(c):
        for h in range(pair):
            for d in range(1, major):
                a2_copy(c, h, d).wait_recv()
        if c == 0:
            for copy in weights[:experts]:
                copy.wait()
        for j in range(experts):
            low_g, high_g = spans[j]
            rows = (high_g - low_g) * 8
            for b, (h, i, k) in enumerate(blocks):
                piece = buf[c, h, i, k, low_g:high_g].astype(jnp.float32)
                xs[j, b * rows : (b + 1) * rows] = piece.reshape(rows, width).astype(jnp.bfloat16)
        tile = 256 if hidden % 256 == 0 else hidden

        def first(n, carry):
            cols = pl.ds(pl.multiple_of(n * tile, tile), tile) if tile < hidden else slice(None)
            for j in range(experts):
                rows = (spans[j][1] - spans[j][0]) * 8 * len(blocks)
                acc = jnp.dot(
                    xs[j, :rows], w1[j, :, cols], preferred_element_type=jnp.float32
                )
                acc = acc + b_in_ref[j : j + 1, cols]
                acc = 0.5 * acc * (1.0 + lax.erf(acc * math.sqrt(0.5)))
                hs[j, :rows, cols] = acc.astype(jnp.bfloat16)
            return carry

        lax.fori_loop(0, hidden // tile, first, 0)
        if c == 0:
            for copy in weights[experts:]:
                copy.wait()
        wide = 256 if width % 256 == 0 else width

        def second(n, carry):
            cols = pl.ds(pl.multiple_of(n * wide, wide), wide) if wide < width else slice(None)
            outs = []
            for j in range(experts):
                rows = (spans[j][1] - spans[j][0]) * 8 * len(blocks)
                acc = jnp.dot(
                    hs[j, :rows], w2[j, :, cols], preferred_element_type=jnp.float32
                )
                outs.append(acc.reshape(len(blocks), spans[j][1] - spans[j][0], 8, wide))
            line = lax.broadcasted_iota(jnp.int32, (8, wide), 0)
            for b, (h, i, k) in enumerate(blocks):
                for g in range(groups):
                    value = None
                    for j in range(experts):
                        if spans[j][0] <= g < spans[j][1]:
                            mine = outs[j][b, g - spans[j][0]]
                            if value is None:
                                value = mine
                            else:
                                value = jnp.where(line + g * 8 < j * slot, value, mine)
                    part[c, h, i, k, g, :, cols] = value.astype(jnp.bfloat16)
            return carry

        lax.fori_loop(0, width // wide, second, 0)
        for h in range(pair):
            for d in range(1, major):
                r1_copy(c, h, d).start()

    def reduce_far(c):
        for h in range(pair):
            maj, low = place(h)
            for d in range(1, major):
                r1_copy(c, h, d).wait_recv()
            for k in range(minor):
                for g in range(groups):
                    total = part[c, h, maj, k, g].astype(jnp.float32)
                    for d in range(1, major):
                        total = total + got1[c, h, d - 1, k, g].astype(jnp.float32)
                    red[c, h, k, g] = total.astype(jnp.bfloat16)
            for d in range(1, minor):
                r2_copy(c, h, d).start()

    def reduce_near(c):
        line = lax.broadcasted_iota(jnp.int32, (8, width), 0)
        for h in range(pair):
            maj, low = place(h)
            for d in range(1, minor):
                r2_copy(c, h, d).wait_recv()
            for g in range(groups):
                total = red[c, h, low, g].astype(jnp.float32)
                for d in range(1, minor):
                    total = total + got2[c, h, d - 1, g].astype(jnp.float32)
                bias = jnp.broadcast_to(b_out_ref[0:1, :], (8, width))
                for j in range(1, experts):
                    bias = jnp.where(line + g * 8 < j * slot, bias, b_out_ref[j : j + 1, :])
                value = (total + bias).astype(jnp.bfloat16)
                if c == 0 and h == 0:
                    out_ref[me_e, g] = value
                else:
                    fin[c, h, g] = value
            if not (c == 0 and h == 0):
                b_copy(c, h).start()

    own.start()
    for c in range(n_chunk):
        for h in range(pair):
            if not (c == 0 and h == 0):
                z_copy(c, h).start()
        if c == 0:
            for copy in weights:
                copy.start()
    stages = ((gather_near, 0), (gather_far, 1), (compute, 2), (reduce_far, 3), (reduce_near, 4))
    for t in range(n_chunk + 4):
        for stage, lag in stages:
            if 0 <= t - lag < n_chunk:
                stage(t - lag)
    for c in range(n_chunk):
        for h in range(pair):
            if not (c == 0 and h == 0):
                b_copy(c, h).wait_recv()
                b_copy(c, h).wait_send()
                z_copy(c, h).wait_send()
            for d in range(1, minor):
                a1_copy(c, h, d).wait_send()
                r2_copy(c, h, d).wait_send()
            for d in range(1, major):
                a2_copy(c, h, d).wait_send()
                r1_copy(c, h, d).wait_send()


def expert_exchange(sent, w_in, b_in, w_out, b_out, n_seq, slot):
    n_exp, groups, _, width = sent.shape
    experts, _, hidden = w_in.shape
    pair = 2 if n_exp % 2 == 0 else 1
    n_chunk = n_exp // pair
    side = math.isqrt(n_seq)
    major, minor = (side, side) if side * side == n_seq else (1, n_seq)
    dims = (n_seq, n_exp, n_chunk, pair, major, minor, experts, slot)
    block = (groups, 8, width)
    bf = jnp.bfloat16
    tallest = max(-(-(j + 1) * slot // 8) - j * slot // 8 for j in range(experts)) * 8
    rows = tallest * pair * n_seq
    sem = pltpu.SemaphoreType.DMA
    vmem = pl.BlockSpec(memory_space=pltpu.VMEM)
    hbm = pl.BlockSpec(memory_space=pl.ANY)
    return pl.pallas_call(
        functools.partial(exchange_kernel, dims),
        out_shape=jax.ShapeDtypeStruct(sent.shape, bf),
        in_specs=[vmem, vmem, vmem, hbm, hbm],
        out_specs=vmem,
        scratch_shapes=[
            pltpu.VMEM(w_in.shape, bf),
            pltpu.VMEM(w_out.shape, bf),
            pltpu.VMEM((n_chunk, pair, major, minor) + block, bf),
            pltpu.VMEM((n_chunk, pair, major, minor) + block, bf),
            pltpu.VMEM((n_chunk, pair, max(major - 1, 1), minor) + block, bf),
            pltpu.VMEM((n_chunk, pair, minor) + block, bf),
            pltpu.VMEM((n_chunk, pair, max(minor - 1, 1)) + block, bf),
            pltpu.VMEM((n_chunk, pair) + block, bf),
            pltpu.VMEM((experts, rows, width), bf),
            pltpu.VMEM((experts, rows, hidden), bf),
            sem((2, experts)),
            sem,
            sem((n_chunk, pair)),
            sem((n_chunk, pair)),
            sem((n_chunk, pair, minor)),
            sem((n_chunk, pair, minor)),
            sem((n_chunk, pair, major)),
            sem((n_chunk, pair, major)),
            sem((n_chunk, pair, major)),
            sem((n_chunk, pair, major)),
            sem((n_chunk, pair, minor)),
            sem((n_chunk, pair, minor)),
            sem((n_chunk, pair)),
            sem((n_chunk, pair)),
        ],
        compiler_params=pltpu.CompilerParams(
            collective_id=0, has_side_effects=True, vmem_limit_bytes=VMEM_LIMIT
        ),
        cost_estimate=pl.CostEstimate(
            flops=4 * experts * rows * width * hidden,
            bytes_accessed=4 * experts * width * hidden,
            transcendentals=experts * rows * hidden,
        ),
    )(sent, b_in, b_out, w_in, w_out)


def body(
    tokens,
    expert_ids,
    gate_values,
    mixer_gain,
    expert_gain,
    conv_weight,
    conv_bias,
    w_in,
    b_in,
    w_out,
    b_out,
):
    row_count = tokens.shape[1]
    col_count = tokens.shape[2]
    width_d = tokens.shape[3]
    values = tokens[0].astype(jnp.float32)
    normed = normalize(values, mixer_gain).astype(jnp.bfloat16)
    rim_source = tokens[0]
    extended = with_halo(rim_source, (("seq", 0),), 1)
    rim_rows = jnp.concatenate([extended[0:1], extended[row_count + 1 : row_count + 2]], axis=0)
    rim_rows = normalize(rim_rows.astype(jnp.float32), mixer_gain).astype(jnp.bfloat16)
    extended = jnp.concatenate([rim_rows[0:1], normed, rim_rows[1:2]], axis=0)
    padded = jnp.pad(extended.astype(jnp.float32), ((0, 0), (1, 1), (0, 0)))
    mixed = values + depthwise(padded, conv_weight, row_count, col_count) + conv_bias
    tok_rows = row_count * col_count
    expert_in = normalize(mixed, expert_gain).astype(jnp.bfloat16).reshape(tok_rows, width_d)
    per_device = w_in.shape[0]
    holders = lax.axis_size("exp")
    experts = per_device * holders
    slot_count = 5 * tok_rows // (4 * experts)
    block_rows = -(-per_device * slot_count // 8) * 8
    route_ids = expert_ids.reshape(tok_rows)
    one_hot = (route_ids[:, None] == jnp.arange(experts, dtype=jnp.int32)[None, :]).astype(
        jnp.bfloat16
    )
    positions = jnp.arange(tok_rows, dtype=jnp.int32)
    below_mask = (positions[:, None] > positions[None, :]).astype(jnp.bfloat16)
    earlier = jnp.dot(below_mask, one_hot, preferred_element_type=jnp.float32)
    slot_rank = jnp.sum(earlier * one_hot.astype(jnp.float32), axis=1).astype(jnp.int32)
    column = (
        route_ids // per_device * block_rows + route_ids % per_device * slot_count + slot_rank
    )
    dispatch_mask = (
        column[:, None] == jnp.arange(holders * block_rows, dtype=jnp.int32)[None, :]
    ).astype(jnp.bfloat16)
    dispatched = jnp.einsum(
        "tk,td->kd", dispatch_mask, expert_in, preferred_element_type=jnp.float32
    ).astype(jnp.bfloat16)
    returned = expert_exchange(
        dispatched.reshape(holders, block_rows // 8, 8, width_d),
        w_in,
        b_in,
        w_out,
        b_out,
        lax.axis_size("seq"),
        slot_count,
    ).reshape(holders * block_rows, width_d)
    combined = jnp.dot(dispatch_mask, returned, preferred_element_type=jnp.float32)
    result = mixed.reshape(tok_rows, width_d) + gate_values.reshape(tok_rows)[:, None] * combined
    return result.astype(jnp.bfloat16).reshape(tokens.shape)


def solution(mesh):
    in_specs = (
        P(("dp", "exp"), "seq", None, None),
        P(("dp", "exp"), "seq", None, None),
        P(("dp", "exp"), "seq", None),
        P(),
        P(),
        P(),
        P(),
        P("exp", None, "seq"),
        P("exp", "seq"),
        P("exp", "seq", None),
        P("exp", None),
    )
    out_specs = P(("dp", "exp"), "seq", None, None)
    return jax.shard_map(body, mesh=mesh, in_specs=in_specs, out_specs=out_specs, check_vma=False)
```

```python
import functools
import math

import jax
import jax.numpy as jnp
from jax import lax
from jax.experimental import pallas as pl
from jax.experimental.pallas import tpu as pltpu
from jax.sharding import PartitionSpec as P


VMEM_LIMIT = 67_000_000
MESH = pl.DeviceIdType.MESH


def exchange_kernel(
    dims,
    tok_ref,
    ids_ref,
    gain1_ref,
    gain2_ref,
    taps_ref,
    conv_bias_ref,
    b_in_ref,
    b_out_ref,
    w_in_ref,
    w_out_ref,
    out_ref,
    column_ref,
    mixed_ref,
    x_ref,
    halo,
    pad,
    mix,
    ein,
    w1,
    w2,
    buf,
    part,
    got1,
    red,
    got2,
    xs,
    hs,
    w_sem,
    own_sem,
    z_send,
    z_recv,
    a1_send,
    a1_recv,
    a2_send,
    a2_recv,
    r1_send,
    r1_recv,
    r2_send,
    r2_recv,
    b_send,
    b_recv,
    halo_send,
    halo_recv,
    mix_sem,
):
    n_seq, n_exp, n_chunk, pair, major, minor, experts, slot = dims
    groups = out_ref.shape[1]
    width = out_ref.shape[3]
    hidden = w1.shape[2]
    me_s = lax.axis_index("seq")
    me_e = lax.axis_index("exp")
    me_z = me_e // pair
    me_c = me_e % pair

    def place(h):
        if major == minor and h % 2 == 1:
            return me_s % minor, me_s // minor
        return me_s // minor, me_s % minor

    def at(h, maj, low):
        if major == minor and h % 2 == 1:
            return low * minor + maj
        return maj * minor + low

    def remote(src, dst, send, recv, seq, exp):
        return pltpu.make_async_remote_copy(
            src_ref=src,
            dst_ref=dst,
            send_sem=send,
            recv_sem=recv,
            device_id={"seq": seq, "exp": exp},
            device_id_type=MESH,
        )

    weights = []
    for j in range(experts):
        weights.append(pltpu.make_async_copy(w_in_ref.at[j], w1.at[j], w_sem.at[0, j]))
    for j in range(experts):
        weights.append(pltpu.make_async_copy(w_out_ref.at[j], w2.at[j], w_sem.at[1, j]))

    barrier = pltpu.get_barrier_semaphore()
    greeted = 0
    for d in range(1, n_exp):
        pl.semaphore_signal(
            barrier,
            inc=1,
            device_id={"seq": me_s, "exp": (me_e + d) % n_exp},
            device_id_type=MESH,
        )
        greeted += 1
    for h in range(min(pair, 2) if major == minor else 1):
        maj, low = place(h)
        for d in range(1, minor):
            pl.semaphore_signal(
                barrier,
                inc=1,
                device_id={"seq": at(h, maj, (low + d) % minor), "exp": me_e},
                device_id_type=MESH,
            )
            greeted += 1
        if pair == 1:
            for d in range(1, major):
                pl.semaphore_signal(
                    barrier,
                    inc=1,
                    device_id={"seq": at(h, (maj + d) % major, low), "exp": me_e},
                    device_id_type=MESH,
                )
                greeted += 1
    for d in (1, n_seq - 1):
        pl.semaphore_signal(
            barrier,
            inc=1,
            device_id={"seq": (me_s + d) % n_seq, "exp": me_e},
            device_id_type=MESH,
        )
        greeted += 1
    for copy in weights:
        copy.start()
    pl.semaphore_wait(barrier, greeted)

    def z_copy(c, h):
        target = (me_z + c) % n_chunk * pair + (me_c + pair - h) % pair
        maj, low = place(h)
        return remote(
            x_ref.at[target],
            buf.at[c, h, maj, low],
            z_send.at[c, h],
            z_recv.at[c, h],
            me_s,
            target,
        )

    own_maj, own_low = place(0)
    own = pltpu.make_async_copy(x_ref.at[me_e], buf.at[0, 0, own_maj, own_low], own_sem)

    def a1_copy(c, h, d):
        maj, low = place(h)
        block = buf.at[c, h, maj, low]
        return remote(
            block,
            block,
            a1_send.at[c, h, d],
            a1_recv.at[c, h, d],
            at(h, maj, (low + d) % minor),
            me_e,
        )

    def a2_copy(c, h, d):
        maj, low = place(h)
        block = buf.at[c, h, maj]
        return remote(
            block,
            block,
            a2_send.at[c, h, d],
            a2_recv.at[c, h, d],
            at(h, (maj + d) % major, low),
            me_e,
        )

    def r1_copy(c, h, d):
        maj, low = place(h)
        return remote(
            part.at[c, h, (maj + d) % major],
            got1.at[c, h, d - 1],
            r1_send.at[c, h, d],
            r1_recv.at[c, h, d],
            at(h, (maj + d) % major, low),
            me_e,
        )

    def r2_copy(c, h, d):
        maj, low = place(h)
        return remote(
            red.at[c, h, (low + d) % minor],
            got2.at[c, h, d - 1],
            r2_send.at[c, h, d],
            r2_recv.at[c, h, d],
            at(h, maj, (low + d) % minor),
            me_e,
        )

    def b_copy(c, h):
        target = (me_z + n_chunk - c) % n_chunk * pair + (me_c + h) % pair
        return remote(
            red.at[c, h, place(h)[1]],
            out_ref.at[me_e],
            b_send.at[c, h],
            b_recv.at[c, h],
            me_s,
            target,
        )

    def gather_near(c):
        for h in range(pair):
            if c == 0 and h == 0:
                own.wait()
            else:
                z_copy(c, h).wait_recv()
            for d in range(1, minor):
                a1_copy(c, h, d).start()

    def gather_far(c):
        for h in range(pair):
            for d in range(1, minor):
                a1_copy(c, h, d).wait_recv()
            for d in range(1, major):
                a2_copy(c, h, d).start()

    spans = []
    for j in range(experts):
        spans.append((j * slot // 8, -(-(j + 1) * slot // 8)))

    blocks = [(h, i, k) for h in range(pair) for i in range(major) for k in range(minor)]

    def compute(c):
        for h in range(pair):
            for d in range(1, major):
                a2_copy(c, h, d).wait_recv()
        if c == 0:
            for copy in weights[:experts]:
                copy.wait()
        for j in range(experts):
            low_g, high_g = spans[j]
            rows = (high_g - low_g) * 8
            for b, (h, i, k) in enumerate(blocks):
                piece = buf[c, h, i, k, low_g:high_g].astype(jnp.float32)
                xs[j, b * rows : (b + 1) * rows] = piece.reshape(rows, width).astype(jnp.bfloat16)
        tile = 256 if hidden % 256 == 0 else hidden

        def first(n, carry):
            cols = pl.ds(pl.multiple_of(n * tile, tile), tile) if tile < hidden else slice(None)
            for j in range(experts):
                rows = (spans[j][1] - spans[j][0]) * 8 * len(blocks)
                acc = jnp.dot(
                    xs[j, :rows], w1[j, :, cols], preferred_element_type=jnp.float32
                )
                acc = acc + b_in_ref[j : j + 1, cols]
                acc = 0.5 * acc * (1.0 + lax.erf(acc * math.sqrt(0.5)))
                hs[j, :rows, cols] = acc.astype(jnp.bfloat16)
            return carry

        lax.fori_loop(0, hidden // tile, first, 0)
        if c == 0:
            for copy in weights[experts:]:
                copy.wait()
        wide = 256 if width % 256 == 0 else width

        def second(n, carry):
            cols = pl.ds(pl.multiple_of(n * wide, wide), wide) if wide < width else slice(None)
            outs = []
            for j in range(experts):
                rows = (spans[j][1] - spans[j][0]) * 8 * len(blocks)
                acc = jnp.dot(
                    hs[j, :rows], w2[j, :, cols], preferred_element_type=jnp.float32
                )
                outs.append(acc.reshape(len(blocks), spans[j][1] - spans[j][0], 8, wide))
            line = lax.broadcasted_iota(jnp.int32, (8, wide), 0)
            for b, (h, i, k) in enumerate(blocks):
                for g in range(groups):
                    value = None
                    for j in range(experts):
                        if spans[j][0] <= g < spans[j][1]:
                            mine = outs[j][b, g - spans[j][0]]
                            if value is None:
                                value = mine
                            else:
                                value = jnp.where(line + g * 8 < j * slot, value, mine)
                    part[c, h, i, k, g, :, cols] = value.astype(jnp.bfloat16)
            return carry

        lax.fori_loop(0, width // wide, second, 0)

    def send_far(c):
        for h in range(pair):
            for d in range(1, major):
                r1_copy(c, h, d).start()

    def reduce_far(c):
        for h in range(pair):
            maj, low = place(h)
            for d in range(1, major):
                r1_copy(c, h, d).wait_recv()
            for k in range(minor):
                for g in range(groups):
                    total = part[c, h, maj, k, g].astype(jnp.float32)
                    for d in range(1, major):
                        total = total + got1[c, h, d - 1, k, g].astype(jnp.float32)
                    red[c, h, k, g] = total.astype(jnp.bfloat16)
            for d in range(1, minor):
                r2_copy(c, h, d).start()

    def reduce_near(c):
        line = lax.broadcasted_iota(jnp.int32, (8, width), 0)
        for h in range(pair):
            maj, low = place(h)
            for d in range(1, minor):
                r2_copy(c, h, d).wait_recv()
            for g in range(groups):
                total = red[c, h, low, g].astype(jnp.float32)
                for d in range(1, minor):
                    total = total + got2[c, h, d - 1, g].astype(jnp.float32)
                bias = jnp.broadcast_to(b_out_ref[0:1, :], (8, width))
                for j in range(1, experts):
                    bias = jnp.where(line + g * 8 < j * slot, bias, b_out_ref[j : j + 1, :])
                value = (total + bias).astype(jnp.bfloat16)
                if c == 0 and h == 0:
                    out_ref[me_e, g] = value
                else:
                    red[c, h, low, g] = value
            if not (c == 0 and h == 0):
                b_copy(c, h).start()

    row_count, cols = tok_ref.shape[0], tok_ref.shape[1]
    halos = [
        remote(
            tok_ref.at[row_count - 1],
            halo.at[0],
            halo_send.at[0],
            halo_recv.at[0],
            (me_s + 1) % n_seq,
            me_e,
        ),
        remote(
            tok_ref.at[0],
            halo.at[1],
            halo_send.at[1],
            halo_recv.at[1],
            (me_s + n_seq - 1) % n_seq,
            me_e,
        ),
    ]
    for copy in halos:
        copy.start()

    step = 16

    def norm(values, scales):
        mean = jnp.mean(values, axis=-1, keepdims=True)
        centred = values - mean
        var = jnp.mean(centred * centred, axis=-1, keepdims=True)
        return (centred * lax.rsqrt(var + 1e-06) * scales).astype(jnp.bfloat16)

    edge = jnp.zeros((8, width), jnp.float32)

    def norm_row(r, carry):
        pad[r + 1, 0:8] = edge
        pad[r + 1, cols + 8 : cols + 16] = edge
        for q in range(cols // step):
            piece = tok_ref[r, q * step : (q + 1) * step].astype(jnp.float32)
            pad[r + 1, 8 + q * step : 8 + (q + 1) * step] = norm(piece, gain1_ref[...]).astype(
                jnp.float32
            )
        return carry

    lax.fori_loop(0, row_count, norm_row, 0)

    def mix_row(r, carry):
        for q in range(cols // step):
            total = tok_ref[r, q * step : (q + 1) * step].astype(jnp.float32)
            total = total + conv_bias_ref[...]
            for a in range(3):
                for b in range(3):
                    low = 7 + b + q * step
                    tap = taps_ref[3 * a + b : 3 * a + b + 1, :]
                    total = total + pad[r + a, low : low + step] * tap
            where = pl.ds(pl.multiple_of(r * cols + q * step, step), step)
            mix[where, :] = total
            ein[where, :] = norm(total, gain2_ref[...])
        return carry

    tok_rows = ids_ref.shape[1]
    total_experts = experts * n_exp
    ids = ids_ref[...]
    names = lax.broadcasted_iota(jnp.int32, (total_experts, tok_rows), 0)
    one_hot = jnp.where(names == ids, 1.0, 0.0)
    before = lax.broadcasted_iota(jnp.int32, (tok_rows, tok_rows), 0)
    after = lax.broadcasted_iota(jnp.int32, (tok_rows, tok_rows), 1)
    earlier = jnp.dot(
        one_hot.astype(jnp.bfloat16),
        jnp.where(before < after, 1.0, 0.0).astype(jnp.bfloat16),
        preferred_element_type=jnp.float32,
    )
    rank = jnp.sum(one_hot * earlier, axis=0, keepdims=True)
    ids_f = ids.astype(jnp.float32)
    holder = jnp.floor((ids_f + 0.5) * (1.0 / experts))
    column = holder * (groups * 8.0) + (ids_f - holder * experts) * (1.0 * slot) + rank
    column_ref[...] = column

    lax.fori_loop(1, row_count - 1, mix_row, 0)
    for side, copy in enumerate(halos):
        copy.wait_recv()
    ends = (me_s > 0, me_s < n_seq - 1)
    for side, r in ((0, 0), (1, row_count + 1)):
        keep = jnp.where(ends[side], 1.0, 0.0).astype(jnp.float32)
        pad[r, 0:8] = edge
        pad[r, cols + 8 : cols + 16] = edge
        for q in range(cols // step):
            piece = halo[side, q * step : (q + 1) * step].astype(jnp.float32)
            pad[r, 8 + q * step : 8 + (q + 1) * step] = (
                norm(piece, gain1_ref[...]).astype(jnp.float32) * keep
            )
    for r in range(0, row_count, max(row_count - 1, 1)):
        mix_row(r, 0)
    keep_mix = pltpu.make_async_copy(mix, mixed_ref, mix_sem)
    keep_mix.start()

    height = groups * 8
    for c in range(n_chunk):
        targets = [
            (me_z + c) % n_chunk * pair + (me_c + pair - h) % pair for h in range(pair)
        ]
        line = lax.broadcasted_iota(jnp.int32, (pair * height, tok_rows), 0)
        name = line + targets[0] * height
        for h in range(1, pair):
            name = jnp.where(line < h * height, name, line + (targets[h] - h) * height)
        mask = jnp.where(name.astype(jnp.float32) == column, 1.0, 0.0).astype(jnp.bfloat16)
        picked = jnp.dot(mask, ein[...], preferred_element_type=jnp.float32)
        for h in range(pair):
            piece = picked[h * height : (h + 1) * height].reshape(groups, 8, width)
            x_ref[targets[h]] = piece.astype(jnp.bfloat16)
            if c == 0 and h == 0:
                own.start()
            else:
                z_copy(c, h).start()

    send_order = list(range(1, n_chunk)) + [0]
    events = [(0.0, gather_near, 0)]
    for c in range(1, n_chunk):
        events.append((c, gather_near, c))
    for c in range(n_chunk):
        events.append((c + 0.9, gather_far, c))
        events.append((c + 2.3, compute, c))
    for n, c in enumerate(send_order):
        events.append((n + 3.4 if c else n_chunk + 1.5, send_far, c))
        events.append((n + 4.5, reduce_far, c))
        events.append((n + 5.6, reduce_near, c))
    for _, stage, c in sorted(events, key=lambda event: event[0]):
        stage(c)
    keep_mix.wait()
    for copy in halos:
        copy.wait_send()
    for c in range(n_chunk):
        for h in range(pair):
            if not (c == 0 and h == 0):
                b_copy(c, h).wait_recv()
                b_copy(c, h).wait_send()
                z_copy(c, h).wait_send()
            for d in range(1, minor):
                a1_copy(c, h, d).wait_send()
                r2_copy(c, h, d).wait_send()
            for d in range(1, major):
                a2_copy(c, h, d).wait_send()
                r1_copy(c, h, d).wait_send()


def expert_exchange(front, w_in, b_in, w_out, b_out, n_seq, n_exp, slot):
    row_count, cols, width = front[0].shape
    tok_rows = row_count * cols
    groups = -(-w_in.shape[0] * slot // 8)
    experts, _, hidden = w_in.shape
    pair = 2 if n_exp % 2 == 0 else 1
    n_chunk = n_exp // pair
    side = math.isqrt(n_seq)
    major, minor = (side, side) if side * side == n_seq else (1, n_seq)
    dims = (n_seq, n_exp, n_chunk, pair, major, minor, experts, slot)
    block = (groups, 8, width)
    bf = jnp.bfloat16
    tallest = max(-(-(j + 1) * slot // 8) - j * slot // 8 for j in range(experts)) * 8
    rows = tallest * pair * n_seq
    sem = pltpu.SemaphoreType.DMA
    vmem = pl.BlockSpec(memory_space=pltpu.VMEM)
    hbm = pl.BlockSpec(memory_space=pl.ANY)
    return pl.pallas_call(
        functools.partial(exchange_kernel, dims),
        out_shape=(
            jax.ShapeDtypeStruct((n_exp,) + block, bf),
            jax.ShapeDtypeStruct((1, tok_rows), jnp.float32),
            jax.ShapeDtypeStruct((tok_rows, width), jnp.float32),
        ),
        in_specs=[vmem] * 8 + [hbm, hbm],
        out_specs=(vmem, vmem, hbm),
        scratch_shapes=[
            pltpu.VMEM((n_exp,) + block, bf),
            pltpu.VMEM((2, cols, width), bf),
            pltpu.VMEM((row_count + 2, cols + 16, width), jnp.float32),
            pltpu.VMEM((tok_rows, width), jnp.float32),
            pltpu.VMEM((tok_rows, width), bf),
            pltpu.VMEM(w_in.shape, bf),
            pltpu.VMEM(w_out.shape, bf),
            pltpu.VMEM((n_chunk, pair, major, minor) + block, bf),
            pltpu.VMEM((n_chunk, pair, major, minor) + block, bf),
            pltpu.VMEM((n_chunk, pair, max(major - 1, 1), minor) + block, bf),
            pltpu.VMEM((n_chunk, pair, minor) + block, bf),
            pltpu.VMEM((n_chunk, pair, max(minor - 1, 1)) + block, bf),
            pltpu.VMEM((experts, rows, width), bf),
            pltpu.VMEM((experts, rows, hidden), bf),
            sem((2, experts)),
            sem,
            sem((n_chunk, pair)),
            sem((n_chunk, pair)),
            sem((n_chunk, pair, minor)),
            sem((n_chunk, pair, minor)),
            sem((n_chunk, pair, major)),
            sem((n_chunk, pair, major)),
            sem((n_chunk, pair, major)),
            sem((n_chunk, pair, major)),
            sem((n_chunk, pair, minor)),
            sem((n_chunk, pair, minor)),
            sem((n_chunk, pair)),
            sem((n_chunk, pair)),
            sem((2,)),
            sem((2,)),
            sem,
        ],
        compiler_params=pltpu.CompilerParams(
            collective_id=0, has_side_effects=True, vmem_limit_bytes=VMEM_LIMIT
        ),
        cost_estimate=pl.CostEstimate(
            flops=4 * experts * rows * width * hidden,
            bytes_accessed=4 * experts * width * hidden,
            transcendentals=experts * rows * hidden,
        ),
    )(*front, b_in, b_out, w_in, w_out)


def body(
    tokens,
    expert_ids,
    gate_values,
    mixer_gain,
    expert_gain,
    conv_weight,
    conv_bias,
    w_in,
    b_in,
    w_out,
    b_out,
):
    row_count = tokens.shape[1]
    col_count = tokens.shape[2]
    width_d = tokens.shape[3]
    tok_rows = row_count * col_count
    per_device = w_in.shape[0]
    holders = lax.axis_size("exp")
    experts = per_device * holders
    slot_count = 5 * tok_rows // (4 * experts)
    block_rows = -(-per_device * slot_count // 8) * 8
    front = (
        tokens[0],
        expert_ids.reshape(1, tok_rows),
        mixer_gain.reshape(1, width_d),
        expert_gain.reshape(1, width_d),
        conv_weight.reshape(9, width_d),
        conv_bias.reshape(1, width_d),
    )
    returned, column, mixed = expert_exchange(
        front, w_in, b_in, w_out, b_out, lax.axis_size("seq"), holders, slot_count
    )
    returned = returned.reshape(holders * block_rows, width_d)
    dispatch_mask = (
        column.reshape(tok_rows)[:, None]
        == jnp.arange(holders * block_rows, dtype=jnp.float32)[None, :]
    ).astype(jnp.bfloat16)
    combined = jnp.dot(dispatch_mask, returned, preferred_element_type=jnp.float32)
    result = mixed.reshape(tok_rows, width_d) + gate_values.reshape(tok_rows)[:, None] * combined
    return result.astype(jnp.bfloat16).reshape(tokens.shape)


def solution(mesh):
    in_specs = (
        P(("dp", "exp"), "seq", None, None),
        P(("dp", "exp"), "seq", None, None),
        P(("dp", "exp"), "seq", None),
        P(),
        P(),
        P(),
        P(),
        P("exp", None, "seq"),
        P("exp", "seq"),
        P("exp", "seq", None),
        P("exp", None),
    )
    out_specs = P(("dp", "exp"), "seq", None, None)
    return jax.shard_map(body, mesh=mesh, in_specs=in_specs, out_specs=out_specs, check_vma=False)
```
